32 devices in a mesh: cp: 8 (over z, y), fs: 4 (over x, core).
Axes of the slice: x: 2, y: 2, z: 4, core: 2. Of those that a mesh axis runs over, the one named last changes fastest.
Arguments:
- embeds: bfloat16 [4, 2048, 4096], P('fs', 'cp'), may hold values from -6 to 6
- queries: bfloat16 [4, 2048, 2048], P('fs', 'cp'), may hold values from -12 to 12
- key_heads: bfloat16 [4, 2048, 512], P('fs', 'cp'), may hold values from -4 to 4
- cotangent: bfloat16 [4, 2048, 2048], P('fs', 'cp'), may hold values from -6 to 6
- doc_start: int32 [4, 2048], P('fs', 'cp'), may hold values from 0 to 2047, as said below
- need_ids: int32 [4, 8, 5], P('fs', 'cp'), may hold values from -1 to 7, as said below
- y_weight: bfloat16 [4096, 512], P(('cp', 'fs')), may hold values from -0.09375 to 0.09375
- z_weight: float32 [4096, 512], P(('cp', 'fs')), may hold values from -0.09375 to 0.09375
- x_weight: float32 [4096, 512], P(('cp', 'fs')), may hold values from -0.09375 to 0.09375
- second_moment: float32 [4096, 512], P(('cp', 'fs')), may hold values from 1e-05 to 0.001
Outputs:
- z_next: float32 [4096, 512], P(('cp', 'fs'))
- x_next: float32 [4096, 512], P(('cp', 'fs'))
- moment_next: float32 [4096, 512], P(('cp', 'fs'))
- y_next: bfloat16 [4096, 512], P(('cp', 'fs'))
The draws below stay inside these ranges and needn't reach their ends.
Inputs may be any that keep to these rules, and one draw needn't show every extreme that they name: `doc_start`: documents are contiguous and hold at most 1024 tokens, so a query block needs key-value blocks at most 4 blocks back; in every sequence some query block needs the block exactly 4 back. need_ids[f, b, j] is b - j when some query of block b is allowed a key of block b - j, else -1; need_ids[f, b, 0] is always b.
All inputs are finite; a program needn't handle non-finite values.
Results may differ from the reference program's by a relative error of at most 0.0027.
The reference program's roundings to bfloat16 on the way count: a program that leaves them out, or rounds other values in their place, can miss the bound.
Values may be sent and summed in bfloat16 or wider, within the bound.
A program may use at most 128 MiB of HBM per device.

```python
import math
import jax
import jax.numpy as jnp
from jax import lax

D = 4096
HEAD = 128
KV_HEADS = 4
TOK_DEV = 256
WIN = 4
GROUP = 4
QW = 2048
E = 512
SEQ = 2048
N_CP = 8
N_FS = 4


def query_and_key(key):
    seq_len = TOK_DEV * N_CP
    key_draw = jnp.clip(jax.random.normal(jax.random.fold_in(key, 31), (N_FS, seq_len, E), jnp.float32), -4.0, 4.0)
    query_draw = jnp.clip(jax.random.normal(jax.random.fold_in(key, 32), (N_FS, seq_len, QW), jnp.float32), -6.0, 6.0)
    return (key_draw, query_draw)


def document_starts(key):
    seq_len = TOK_DEV * N_CP
    half_block = TOK_DEV // 2
    span_len = WIN * TOK_DEV
    position = jnp.arange(seq_len, dtype=jnp.int32)
    span_index = jnp.floor_divide(position - half_block, span_len)
    span_first = jnp.maximum(half_block + span_index * span_len, 0)
    span_total = seq_len // span_len + 2
    levels = jax.random.randint(jax.random.fold_in(key, 21), (N_FS, span_total), 0, 4)
    rate_table = jnp.array([0, 2, 8, 32], jnp.int32)
    cut_rate = rate_table[levels]
    cut_rate = cut_rate.at[:, 1].set(0)
    span_rate = cut_rate[:, span_index + 1]
    coin_draw = jax.random.randint(jax.random.fold_in(key, 22), (N_FS, seq_len), 0, 1024)
    forced_off = jax.random.randint(jax.random.fold_in(key, 23), (N_FS, span_total), 1, span_len)
    span_forced = forced_off[:, span_index + 1]
    forced_cut = ((position - span_first)[None, :] == span_forced) & (span_index != 0)[None, :]
    marker = (position[None, :] == span_first[None, :]) | (coin_draw < span_rate) | forced_cut
    return lax.cummax(jnp.where(marker, position[None, :], 0), axis=1).astype(jnp.int32)


def draw_queries(key, part):
    return query_and_key(key)[1].astype(jnp.bfloat16)


def draw_key_heads(key, part):
    return query_and_key(key)[0].astype(jnp.bfloat16)


def draw_doc_start(key, part):
    return document_starts(key)


def draw_need_ids(key, part):
    starts = document_starts(key)
    first_of_block = starts[:, ::TOK_DEV]
    block_ids = jnp.arange(N_CP, dtype=jnp.int32)[:, None]
    back_steps = jnp.arange(WIN + 1, dtype=jnp.int32)[None, :]
    target = block_ids - back_steps
    needed = (first_of_block[:, :, None] < (target + 1)[None] * TOK_DEV) & (target >= 0)[None]
    return jnp.where(needed, target[None], -1).astype(jnp.int32)


def with_spikes(values, own_key, source, target, blocks, factor):
    def block_of(dim):
        return (jnp.arange(values.shape[dim]) // (values.shape[dim] // blocks)).reshape((-1,) + (1,) * (values.ndim - 1 - dim))

    near = jax.random.permutation(own_key, blocks)[block_of(target)]
    other_side = (block_of(target) + blocks // 2) % blocks
    return jnp.where((block_of(source) == near) | (block_of(source) == other_side), factor * values, values)


def block_scale(own_key, extent, cuts, smallest, high):
    gain, own = 1.0, jax.random.fold_in(own_key, 6)
    for dim, shards_of in cuts:
        steps = jnp.exp(jax.random.uniform(jax.random.fold_in(own, dim), (shards_of,), jnp.float32, smallest / len(cuts), high / len(cuts)))
        gain = gain * jnp.repeat(steps, extent[dim] // shards_of).reshape([-1 if axis == dim else 1 for axis in range(len(extent))])
    return gain


def normal_values(key, extent, width, bound, pieces=(), kind=jnp.bfloat16):
    drawn = width * jax.random.normal(key, extent, jnp.float32)
    if pieces:
        drawn = drawn * block_scale(key, extent, pieces, -0.22, 0.18)
    return jnp.clip(drawn, -bound, bound).astype(kind)


def bell_draw_with(key, dims, scale, most, shards, heavy, kind=jnp.bfloat16):
    values = scale * jax.random.normal(key, dims, jnp.float32)
    if shards:
        values = values * block_scale(key, dims, shards, -0.22, 0.18)
    return jnp.clip(with_spikes(values, jax.random.fold_in(key, 3), *heavy), -most, most).astype(kind)


def setup_inputs(seed: int = 0) -> dict:
    key_of = jax.random.split(jax.random.key(seed), 11)
    return {
        "embeds": bell_draw_with(key_of[0], (N_FS, SEQ, D), 1.0, 6.0, ((0, 4), (1, 8)), (1, 2, 8, 2.0)),
        "queries": draw_queries(jax.random.fold_in(key_of[10], 71), 0),
        "key_heads": draw_key_heads(jax.random.fold_in(key_of[10], 71), 0),
        "cotangent": normal_values(key_of[3], (N_FS, SEQ, QW), 1.0, 6.0, ((0, 4), (1, 8))),
        "doc_start": draw_doc_start(jax.random.fold_in(key_of[10], 71), 0),
        "need_ids": draw_need_ids(jax.random.fold_in(key_of[10], 71), 0),
        "y_weight": normal_values(key_of[6], (D, E), D ** -0.5, 0.09375, ((0, 32),)),
        "z_weight": normal_values(key_of[7], (D, E), D ** -0.5, 0.09375, ((0, 32),), jnp.float32),
        "x_weight": normal_values(key_of[8], (D, E), D ** -0.5, 0.09375, ((0, 32),), jnp.float32),
        "second_moment": jnp.clip(jnp.exp(math.log(0.001) - 4.6051703 * jax.random.uniform(key_of[9], (D, E), jnp.float32) ** block_scale(key_of[9], (D, E), ((0, 32),), -0.2, 0.2)), 9.999999747378752e-06, 0.001),
    }


NORM_EPS = 0.01
MOMENT_DECAY = 0.95
LEARN_RATE = 0.005
WEIGHT_DECAY = 0.1
ADAM_EPS = 1e-08
AVERAGE_MIX = 0.25
INTERP_BETA = 0.9

def visible(doc_rows, need_row, block_id, tok_rows):
    span_rows = (WIN + 1) * tok_rows
    query_pos = block_id * tok_rows + jnp.arange(tok_rows, dtype=jnp.int32)
    key_pos = (block_id - WIN) * tok_rows + jnp.arange(span_rows, dtype=jnp.int32)
    key_block = block_id - WIN + jnp.arange(span_rows, dtype=jnp.int32) // tok_rows
    listed = jnp.any(need_row[None, :] == key_block[:, None], axis=1)
    return (key_pos[None, :] >= doc_rows[:, None]) & (key_pos[None, :] <= query_pos[:, None]) & listed[None, :]

def block_attention(query_rows, key_window, value_window, allowed):
    tok_rows = query_rows.shape[0]
    scaling = 1.0 / math.sqrt(HEAD)
    query_split = query_rows.astype(jnp.float32).reshape(tok_rows, KV_HEADS, GROUP, HEAD)
    prob_list = []
    out_list = []
    for kv_head in range(KV_HEADS):
        key_part = key_window[:, kv_head * HEAD:(kv_head + 1) * HEAD].astype(jnp.float32)
        value_part = value_window[:, kv_head * HEAD:(kv_head + 1) * HEAD].astype(jnp.float32)
        scores = jnp.einsum('tgh,sh->gts', query_split[:, kv_head], key_part) * scaling
        scores = jnp.where(allowed[None], scores, -jnp.inf)
        largest = lax.optimization_barrier(jnp.max(scores, axis=-1, keepdims=True))
        weights = jnp.exp(scores - largest)
        probs_low = (weights / lax.optimization_barrier(jnp.sum(weights, axis=-1, keepdims=True))).astype(jnp.bfloat16)
        prob_list.append(probs_low)
        out_list.append(jnp.einsum('gts,sh->tgh', probs_low.astype(jnp.float32), value_part))
    attended = jnp.stack(out_list, axis=1).reshape(tok_rows, KV_HEADS * GROUP * HEAD)
    return (prob_list, attended)

def norm_backward(attended, cot_rows, token_total):
    square_mean = lax.optimization_barrier(jnp.mean(attended * attended, axis=-1, keepdims=True)) + NORM_EPS
    root_scale = jnp.sqrt(square_mean)
    normed = attended / root_scale
    upstream = cot_rows.astype(jnp.float32) / token_total
    inner = lax.optimization_barrier(jnp.mean(upstream * normed, axis=-1, keepdims=True))
    return ((upstream - normed * inner) / root_scale).astype(jnp.bfloat16)

def window_grads(prob_list, out_grad):
    tok_rows = out_grad.shape[0]
    grad_split = out_grad.astype(jnp.float32).reshape(tok_rows, KV_HEADS, GROUP, HEAD)
    head_parts = []
    for kv_head in range(KV_HEADS):
        head_parts.append(jnp.einsum('gts,tgh->sh', prob_list[kv_head].astype(jnp.float32), grad_split[:, kv_head]))
    return jnp.concatenate(head_parts, axis=1)

def reference(embeds, queries, key_heads, cotangent, doc_start, need_ids, y_weight, z_weight, x_weight, second_moment):
    seq_len = embeds.shape[1]
    tok_rows = seq_len // N_CP
    kv_width = key_heads.shape[2]
    token_total = seq_len * N_FS
    gradient = jnp.zeros((embeds.shape[2], kv_width), jnp.float32)
    for seq_index in range(N_FS):
        tokens_here = embeds[seq_index]
        values = jnp.dot(tokens_here, y_weight, preferred_element_type=jnp.float32).astype(jnp.bfloat16)
        padding = jnp.zeros((WIN * tok_rows, kv_width), jnp.bfloat16)
        keys_padded = jnp.concatenate([padding, key_heads[seq_index]], axis=0)
        values_padded = jnp.concatenate([padding, values], axis=0)
        query_seq = queries[seq_index]
        cot_seq = cotangent[seq_index]
        doc_seq = doc_start[seq_index]
        need_seq = need_ids[seq_index]

        def block_grads(block_id):
            first_row = block_id * tok_rows
            span_rows = (WIN + 1) * tok_rows
            query_rows = lax.dynamic_slice_in_dim(query_seq, first_row, tok_rows, 0)
            cot_rows = lax.dynamic_slice_in_dim(cot_seq, first_row, tok_rows, 0)
            doc_rows = lax.dynamic_slice_in_dim(doc_seq, first_row, tok_rows, 0)
            key_window = lax.dynamic_slice_in_dim(keys_padded, first_row, span_rows, 0)
            value_window = lax.dynamic_slice_in_dim(values_padded, first_row, span_rows, 0)
            allowed = visible(doc_rows, need_seq[block_id], block_id, tok_rows)
            prob_list, attended = block_attention(query_rows, key_window, value_window, allowed)
            out_grad = norm_backward(attended, cot_rows, token_total)
            return window_grads(prob_list, out_grad)
        shares = lax.map(block_grads, jnp.arange(N_CP, dtype=jnp.int32))
        shares = shares.reshape(N_CP, WIN + 1, tok_rows, kv_width)
        summed = jnp.zeros((N_CP, tok_rows, kv_width), jnp.float32)
        for slot_index in range(WIN + 1):
            lag_blocks = WIN - slot_index
            shifted = jnp.concatenate([shares[lag_blocks:, slot_index], jnp.zeros((lag_blocks, tok_rows, kv_width), jnp.float32)], axis=0)
            summed = summed + shifted
        value_grad = summed.reshape(seq_len, kv_width).astype(jnp.bfloat16)
        gradient = gradient + jnp.dot(tokens_here.T, value_grad, preferred_element_type=jnp.float32)
    moment_next = MOMENT_DECAY * second_moment + (1.0 - MOMENT_DECAY) * gradient * gradient
    z_next = z_weight - LEARN_RATE * (gradient / (jnp.sqrt(moment_next) + ADAM_EPS) + WEIGHT_DECAY * y_weight.astype(jnp.float32))
    x_next = (1.0 - AVERAGE_MIX) * x_weight + AVERAGE_MIX * z_next
    y_next = ((1.0 - INTERP_BETA) * z_next + INTERP_BETA * x_next).astype(jnp.bfloat16)
    return (z_next, x_next, moment_next, y_next)
```

```python
import math

import jax
import jax.numpy as jnp
from jax import lax
from jax.experimental import pallas as pl
from jax.experimental.pallas import tpu as pltpu
from jax.sharding import PartitionSpec as P

HEAD = 128
KV_HEADS = 4
WIN = 4
GROUP = 4


NORM_EPS = 0.01
MOMENT_DECAY = 0.95
LEARN_RATE = 0.005
WEIGHT_DECAY = 0.1
ADAM_EPS = 1e-08
AVERAGE_MIX = 0.25
INTERP_BETA = 0.9


MESH = pl.DeviceIdType.MESH
VMEM_LIMIT = 60 * 1024 * 1024


def signal_and_wait(peers):
    barrier = pltpu.get_barrier_semaphore()
    for peer in peers:
        pl.semaphore_signal(barrier, inc=1, device_id=peer, device_id_type=MESH)
    pl.semaphore_wait(barrier, len(peers))


def remote(src, dst, send_sem, recv_sem, peer):
    return pltpu.make_async_remote_copy(
        src_ref=src,
        dst_ref=dst,
        send_sem=send_sem,
        recv_sem=recv_sem,
        device_id=peer,
        device_id_type=MESH,
    )


class Place:
    def __init__(self, cp_count, fs_count):
        self.n, self.m = cp_count, fs_count
        self.c, self.f = lax.axis_index("cp"), lax.axis_index("fs")
        self.pair, self.side = self.c // 2, self.c % 2
        self.half = cp_count // 2
        self.mate_c = self.c + 1 - 2 * self.side
        self.twin_f = self.f + 1 - 2 * (self.f % 2)
        self.mate = {"cp": self.mate_c, "fs": self.f}
        self.twin = {"cp": self.c, "fs": self.twin_f}

    def column_c(self, step):
        return ((self.pair + step) % self.half) * 2 + self.side

    def column(self, step):
        return {"cp": self.column_c(step), "fs": self.f}

    def across_f(self, step):
        return (self.f + 2 * step) % self.m

    def across(self, step):
        return {"cp": self.c, "fs": self.across_f(step)}

    def columns(self):
        return [self.column(d) for d in range(1, self.half)]

    def acrosses(self):
        return [self.across(e) for e in range(1, self.m // 2)]


class Window:
    def __init__(self, place, own, win, send, recv):
        self.p, self.own, self.win, self.send, self.recv = place, own, win, send, recv
        self.rows = own.shape[0]

    def slot(self, back):
        return self.win.at[pl.ds((WIN - back) * self.rows, self.rows)]

    def ahead(self, back):
        p = self.p
        peer = {"cp": jnp.minimum(p.c + back, p.n - 1), "fs": p.f}
        return remote(self.own, self.slot(back), self.send.at[back - 1], self.recv.at[back - 1], peer)

    def to_mate(self, source, back):
        return remote(source, self.slot(back), self.send.at[back - 1], self.recv.at[back - 1], self.p.mate)

    def begin(self):
        p = self.p
        for back in (4, 2):

            @pl.when(p.c + back < p.n)
            def _():
                self.ahead(back).start()

        @pl.when(p.side == 0)
        def _():
            self.to_mate(self.own, 1).start()

    def fill(self):
        p = self.p
        self.win[pl.ds(WIN * self.rows, self.rows), :] = self.own[...]
        for back in range(1, WIN + 1):

            @pl.when(p.c < back)
            def _():
                self.win[pl.ds((WIN - back) * self.rows, self.rows), :] = jnp.zeros(
                    self.own.shape, self.own.dtype
                )

    def relay(self):
        p = self.p

        @pl.when(p.c >= 2)
        def _():
            self.ahead(2).wait_recv()

        @pl.when((p.c >= 2) & (p.side == 1))
        def _():
            self.to_mate(self.slot(2), 1).start()

        @pl.when((p.c >= 2) & (p.side == 0))
        def _():
            self.to_mate(self.slot(2), 3).start()

        @pl.when(p.c >= 4)
        def _():
            self.ahead(4).wait_recv()

        @pl.when((p.c >= 4) & (p.side == 1))
        def _():
            self.to_mate(self.slot(4), 3).start()

    def end(self):
        p = self.p
        for back in (1, 3):

            @pl.when(p.c >= back)
            def _():
                self.to_mate(self.own, back).wait_recv()

        for back in (2, 4):

            @pl.when(p.c + back < p.n)
            def _():
                self.ahead(back).wait_send()

        @pl.when((p.side == 0) | (p.c >= 2))
        def _():
            self.to_mate(self.own, 1).wait_send()

        @pl.when(((p.side == 0) & (p.c >= 2)) | (p.c >= 4))
        def _():
            self.to_mate(self.own, 3).wait_send()


def weight_kernel(n, m, y_ref, k_ref, full_ref, win_ref, send, recv, wsend, wrecv):
    p = Place(n, m)
    rows = y_ref.shape[0]
    half, far = n // 2, m // 2
    signal_and_wait(p.columns() + [p.mate] + p.acrosses() + [p.twin])

    def slot(c, f):
        return full_ref.at[pl.ds(pl.multiple_of((c * m + f) * rows, rows), rows)]

    mate_base = half
    across_base = mate_base + half
    twin_base = across_base + (far - 1) * n
    pending = []

    def push(source, c, f, number, peer):
        copy = remote(source, slot(c, f), send.at[number], recv.at[number], peer)
        copy.start()
        pending.append(copy)

    def arrive(c, f, number):
        remote(slot(c, f), slot(c, f), send.at[number], recv.at[number], p.mate).wait_recv()

    def spread(source, c, order):
        for e in range(1, far):
            push(source, c, p.f, across_base + (e - 1) * n + order, p.across(e))
        push(source, c, p.f, twin_base + order, p.twin)

    for d in range(1, half):
        push(y_ref, p.c, p.f, d, p.column(d))
    push(y_ref, p.c, p.f, mate_base, p.mate)
    spread(y_ref, p.c, 0)
    window = Window(p, k_ref, win_ref, wsend, wrecv)
    window.begin()
    full_ref[pl.ds(pl.multiple_of((p.c * m + p.f) * rows, rows), rows), :] = y_ref[...]
    window.fill()
    for d in range(half):
        if d > 0:
            from_c = p.column_c(half - d)
            arrive(from_c, p.f, d)
            push(slot(from_c, p.f), from_c, p.f, mate_base + d, p.mate)
            spread(slot(from_c, p.f), from_c, 2 * d)
        mate_c = p.column_c(half - d) + 1 - 2 * p.side
        arrive(mate_c, p.f, mate_base + d)
        spread(slot(mate_c, p.f), mate_c, 2 * d + 1)
    window.relay()

    def ordered(order):
        from_c = p.column_c((half - order // 2) % half)
        return from_c if order % 2 == 0 else from_c + 1 - 2 * p.side

    for order in range(n):
        c = ordered(order)
        for e in range(1, far):
            g = (p.f + m - 2 * e) % m
            number = across_base + (e - 1) * n + order
            arrive(c, g, number)
            push(slot(c, g), c, g, twin_base + n + (e - 1) * n + order, p.twin)
    for order in range(n):
        c = ordered(order)
        arrive(c, p.twin_f, twin_base + order)
        for e in range(1, far):
            g = (p.twin_f + m - 2 * e) % m
            arrive(c, g, twin_base + n + (e - 1) * n + order)
    window.end()
    for copy in pending:
        copy.wait_send()


def gather_weight(y_weight, keys, n, m):
    rows, width = y_weight.shape
    tok_rows = keys.shape[0]
    numbers = n + (m // 2 - 1) * n + (m // 2) * n
    return pl.pallas_call(
        lambda *refs: weight_kernel(n, m, *refs),
        out_shape=(
            jax.ShapeDtypeStruct((rows * n * m, width), y_weight.dtype),
            jax.ShapeDtypeStruct(((WIN + 1) * tok_rows, width), keys.dtype),
        ),
        in_specs=[pl.BlockSpec(memory_space=pltpu.VMEM)] * 2,
        out_specs=(pl.BlockSpec(memory_space=pltpu.VMEM),) * 2,
        scratch_shapes=[
            pltpu.SemaphoreType.DMA((numbers,)),
            pltpu.SemaphoreType.DMA((numbers,)),
            pltpu.SemaphoreType.DMA((WIN,)),
            pltpu.SemaphoreType.DMA((WIN,)),
        ],
        compiler_params=pltpu.CompilerParams(
            collective_id=1, has_side_effects=True, vmem_limit_bytes=VMEM_LIMIT
        ),
        name="gather_weight",
    )(y_weight, keys)


def column_kernel(n, m, v_ref, e_ref, win_ref, cols_ref, send, recv, wsend, wrecv):
    p = Place(n, m)
    strips, _, _, wide = cols_ref.shape
    others = [{"cp": p.c, "fs": (p.f + e) % m} for e in range(1, m)]
    signal_and_wait(p.columns() + [p.mate] + others)
    window = Window(p, v_ref, win_ref, wsend, wrecv)
    window.begin()

    def strip(k, f):
        return pl.ds(pl.multiple_of((k * m + f) * wide, wide), wide)

    pending = []
    for k in range(strips):
        for e in range(1, m):
            copy = remote(
                e_ref.at[:, strip(k, (p.f + e) % m)],
                cols_ref.at[k, p.f],
                send.at[k * (m - 1) + e - 1],
                recv.at[k * (m - 1) + e - 1],
                others[e - 1],
            )
            copy.start()
            pending.append(copy)
    window.fill()
    for k in range(strips):
        cols_ref[k, p.f] = e_ref[:, strip(k, p.f)]
    window.relay()
    window.end()
    for k in range(strips):
        for e in range(1, m):
            g = (p.f + m - e) % m
            number = k * (m - 1) + e - 1
            remote(
                cols_ref.at[k, g], cols_ref.at[k, g], send.at[number], recv.at[number], others[0]
            ).wait_recv()
    for copy in pending:
        copy.wait_send()


def exchange_columns(values, embeds, strips, wide, n, m):
    tok_rows, width = values.shape
    copies = strips * (m - 1)
    return pl.pallas_call(
        lambda *refs: column_kernel(n, m, *refs),
        out_shape=(
            jax.ShapeDtypeStruct(((WIN + 1) * tok_rows, width), values.dtype),
            jax.ShapeDtypeStruct((strips, m, tok_rows, wide), embeds.dtype),
        ),
        in_specs=[pl.BlockSpec(memory_space=pltpu.VMEM)] * 2,
        out_specs=(pl.BlockSpec(memory_space=pltpu.VMEM),) * 2,
        scratch_shapes=[
            pltpu.SemaphoreType.DMA((copies,)),
            pltpu.SemaphoreType.DMA((copies,)),
            pltpu.SemaphoreType.DMA((WIN,)),
            pltpu.SemaphoreType.DMA((WIN,)),
        ],
        compiler_params=pltpu.CompilerParams(
            collective_id=2, has_side_effects=True, vmem_limit_bytes=VMEM_LIMIT
        ),
        name="exchange_columns",
    )(values, embeds)


CHUNKS = 2


def return_kernel(n, m, own_ref, share_ref, all_ref, got, send, recv, gsend, grecv):
    p = Place(n, m)
    tok_rows = own_ref.shape[0]
    part = tok_rows // CHUNKS
    far = m // 2
    around = []
    for back in range(1, WIN + 1):
        around.append({"cp": (p.c + back) % n, "fs": p.f})
        around.append({"cp": (p.c + n - back) % n, "fs": p.f})
    signal_and_wait(around + p.acrosses() + [p.twin])

    def share(chunk, back):
        rows = pl.ds(chunk * part, part)
        peer = {"cp": jnp.maximum(p.c - back, 0), "fs": p.f}
        number = chunk * WIN + back - 1
        return remote(
            share_ref.at[back - 1, rows], got.at[back - 1, rows], send.at[number], recv.at[number], peer
        )

    for chunk in range(CHUNKS):
        for back in (4, 3, 2, 1):

            @pl.when(p.c >= back)
            def _():
                share(chunk, back).start()

    for back in range(1, WIN + 1):

        @pl.when(p.c + back >= n)
        def _():
            got[back - 1] = jnp.zeros(got.shape[1:], got.dtype)

    def spread(f, chunk, number, peer):
        piece = all_ref.at[f, pl.ds(chunk * part, part)]
        return remote(piece, piece, gsend.at[number], grecv.at[number], peer)

    pending = []
    for chunk in range(CHUNKS):
        base = chunk * (2 * far - 1)
        rows = pl.ds(chunk * part, part)
        for back in range(1, WIN + 1):

            @pl.when(p.c + back < n)
            def _():
                share(chunk, back).wait_recv()

        total = own_ref[rows, :]
        for back in range(1, WIN + 1):
            total = total + got[back - 1, rows, :].astype(jnp.float32)
        all_ref[p.f, rows, :] = total.astype(all_ref.dtype)
        for e in range(1, far):
            pending.append(spread(p.f, chunk, base + e - 1, p.across(e)))
            pending[-1].start()
        pending.append(spread(p.f, chunk, base + far - 1, p.twin))
        pending[-1].start()
    for chunk in range(CHUNKS):
        base = chunk * (2 * far - 1)
        for e in range(1, far):
            g = (p.f + m - 2 * e) % m
            spread(g, chunk, base + e - 1, p.twin).wait_recv()
            pending.append(spread(g, chunk, base + far - 1 + e, p.twin))
            pending[-1].start()
    for chunk in range(CHUNKS):
        base = chunk * (2 * far - 1)
        for e in range(far):
            g = (p.twin_f + m - 2 * e) % m
            spread(g, chunk, base + far - 1 + e, p.twin).wait_recv()
    for copy in pending:
        copy.wait_send()
    for chunk in range(CHUNKS):
        for back in range(1, WIN + 1):

            @pl.when(p.c >= back)
            def _():
                share(chunk, back).wait_send()


def return_shares(own, shares, n, m):
    tok_rows, width = own.shape
    gathers = CHUNKS * (m - 1)
    return pl.pallas_call(
        lambda *refs: return_kernel(n, m, *refs),
        out_shape=jax.ShapeDtypeStruct((m, tok_rows, width), jnp.bfloat16),
        in_specs=[pl.BlockSpec(memory_space=pltpu.VMEM)] * 2,
        out_specs=pl.BlockSpec(memory_space=pltpu.VMEM),
        scratch_shapes=[
            pltpu.VMEM(shares.shape, shares.dtype),
            pltpu.SemaphoreType.DMA((CHUNKS * WIN,)),
            pltpu.SemaphoreType.DMA((CHUNKS * WIN,)),
            pltpu.SemaphoreType.DMA((gathers,)),
            pltpu.SemaphoreType.DMA((gathers,)),
        ],
        compiler_params=pltpu.CompilerParams(
            collective_id=3, has_side_effects=True, vmem_limit_bytes=VMEM_LIMIT
        ),
        name="return_shares",
    )(own, shares)


def reduce_kernel(n, m, part_ref, out_ref, mate_got, sums, got, msend, mrecv, send, recv):
    p = Place(n, m)
    half = n // 2
    signal_and_wait(p.columns() + [p.mate])

    def to_mate(d):
        target = p.column_c(d) + 1 - 2 * p.side
        return remote(part_ref.at[target], mate_got.at[d], msend.at[d], mrecv.at[d], p.mate)

    def to_owner(d):
        return remote(sums.at[d], got.at[d], send.at[d], recv.at[d], p.column(d))

    steps = list(range(half // 2, half)) + list(range(half // 2 - 1, 0, -1)) + [0]
    for d in steps:
        to_mate(d).start()
    for d in steps:
        to_mate(d).wait_recv()
        both = part_ref[p.column_c(d)].astype(jnp.float32) + mate_got[d].astype(jnp.float32)
        if d > 0:
            sums[d] = both.astype(sums.dtype)
            to_owner(d).start()
        else:
            total = both
    for d in range(1, half):
        to_owner(d).wait_recv()
        total = total + got[d].astype(jnp.float32)
    out_ref[...] = total
    for d in range(half):
        to_mate(d).wait_send()
    for d in range(1, half):
        to_owner(d).wait_send()


def reduce_parts(parts, n, m):
    _, rows, width = parts.shape
    half = n // 2
    return pl.pallas_call(
        lambda *refs: reduce_kernel(n, m, *refs),
        out_shape=jax.ShapeDtypeStruct((rows, width), jnp.float32),
        in_specs=[pl.BlockSpec(memory_space=pltpu.VMEM)],
        out_specs=pl.BlockSpec(memory_space=pltpu.VMEM),
        scratch_shapes=[pltpu.VMEM((half, rows, width), parts.dtype)] * 3
        + [pltpu.SemaphoreType.DMA((half,))] * 4,
        compiler_params=pltpu.CompilerParams(
            collective_id=4, has_side_effects=True, vmem_limit_bytes=VMEM_LIMIT
        ),
        name="reduce_parts",
    )(parts)


def visible(doc_rows, need_row, block_id, tok_rows):
    span_rows = (WIN + 1) * tok_rows
    query_pos = block_id * tok_rows + jnp.arange(tok_rows, dtype=jnp.int32)
    key_pos = (block_id - WIN) * tok_rows + jnp.arange(span_rows, dtype=jnp.int32)
    key_block = block_id - WIN + jnp.arange(span_rows, dtype=jnp.int32) // tok_rows
    listed = jnp.any(need_row[None, :] == key_block[:, None], axis=1)
    return (
        (key_pos[None, :] >= doc_rows[:, None])
        & (key_pos[None, :] <= query_pos[:, None])
        & listed[None, :]
    )


def block_attention(query_rows, key_window, value_window, allowed):
    tok_rows = query_rows.shape[0]
    scaling = 1.0 / math.sqrt(HEAD)
    query_split = query_rows.reshape(tok_rows, KV_HEADS, GROUP, HEAD)
    prob_list = []
    out_list = []
    for kv_head in range(KV_HEADS):
        key_part = key_window[:, kv_head * HEAD : (kv_head + 1) * HEAD]
        value_part = value_window[:, kv_head * HEAD : (kv_head + 1) * HEAD]
        scores = (
            jnp.einsum(
                "tgh,sh->gts", query_split[:, kv_head], key_part, preferred_element_type=jnp.float32
            )
            * scaling
        )
        scores = jnp.where(allowed[None], scores, -jnp.inf)
        largest = jnp.max(scores, axis=-1, keepdims=True)
        weights = jnp.exp(scores - largest)
        probs_low = (weights / jnp.sum(weights, axis=-1, keepdims=True)).astype(jnp.bfloat16)
        prob_list.append(probs_low)
        out_list.append(
            jnp.einsum("gts,sh->tgh", probs_low, value_part, preferred_element_type=jnp.float32)
        )
    attended = jnp.stack(out_list, axis=1).reshape(tok_rows, KV_HEADS * GROUP * HEAD)
    return (prob_list, attended)


def norm_backward(attended, cot_rows, token_total):
    square_mean = jnp.mean(attended * attended, axis=-1, keepdims=True) + NORM_EPS
    root_scale = jnp.sqrt(square_mean)
    normed = attended / root_scale
    upstream = cot_rows.astype(jnp.float32) / token_total
    inner = jnp.mean(upstream * normed, axis=-1, keepdims=True)
    return ((upstream - normed * inner) / root_scale).astype(jnp.bfloat16)


def window_grads(prob_list, out_grad):
    tok_rows = out_grad.shape[0]
    grad_split = out_grad.reshape(tok_rows, KV_HEADS, GROUP, HEAD)
    head_parts = []
    for kv_head in range(KV_HEADS):
        head_parts.append(
            jnp.einsum(
                "gts,tgh->sh",
                prob_list[kv_head],
                grad_split[:, kv_head],
                preferred_element_type=jnp.float32,
            )
        )
    return jnp.concatenate(head_parts, axis=1)


def on_device(
    embeds,
    queries,
    key_heads,
    cotangent,
    doc_start,
    need_ids,
    y_weight,
    z_weight,
    x_weight,
    second_moment,
):
    tokens_here = embeds[0]
    tok_rows = tokens_here.shape[0]
    kv_width = key_heads.shape[2]
    block_id = lax.axis_index("cp")
    token_total = tok_rows * lax.axis_size("cp") * lax.axis_size("fs")
    n, m = lax.axis_size("cp"), lax.axis_size("fs")
    own_rows = y_weight.shape[0]
    full_weight, key_window = gather_weight(y_weight, key_heads[0], n, m)
    values = jnp.dot(tokens_here, full_weight, preferred_element_type=jnp.float32).astype(
        jnp.bfloat16
    )
    if own_rows % 128 == 0:
        strips, wide, sent_cols = n, own_rows, tokens_here
    else:
        strips, wide = 1, n * own_rows
        sent_cols = (
            tokens_here.reshape(tok_rows, n, m, own_rows)
            .transpose(0, 2, 1, 3)
            .reshape(tok_rows, n * m * own_rows)
        )
    value_window, group_cols = exchange_columns(values, sent_cols, strips, wide, n, m)
    allowed = visible(doc_start[0], need_ids[0, 0], block_id, tok_rows)
    prob_list, attended = block_attention(queries[0], key_window, value_window, allowed)
    out_grad = norm_backward(attended, cotangent[0], token_total)
    shares = window_grads(prob_list, out_grad).reshape(WIN + 1, tok_rows, kv_width)
    sent_shares = shares[:WIN][::-1].astype(jnp.bfloat16)
    group_grads = return_shares(shares[WIN], sent_shares, n, m)
    parts = jnp.einsum(
        "stw,te->swe",
        group_cols.reshape(strips, m * tok_rows, wide),
        group_grads.reshape(m * tok_rows, kv_width),
        preferred_element_type=jnp.float32,
    ).astype(jnp.bfloat16)
    gradient = reduce_parts(parts.reshape(n, own_rows, kv_width), n, m)
    moment_next = MOMENT_DECAY * second_moment + (1.0 - MOMENT_DECAY) * gradient * gradient
    z_next = z_weight - LEARN_RATE * (
        gradient / (jnp.sqrt(moment_next) + ADAM_EPS) + WEIGHT_DECAY * y_weight.astype(jnp.float32)
    )
    x_next = (1.0 - AVERAGE_MIX) * x_weight + AVERAGE_MIX * z_next
    y_next = ((1.0 - INTERP_BETA) * z_next + INTERP_BETA * x_next).astype(jnp.bfloat16)
    return (z_next, x_next, moment_next, y_next)


def solution(mesh):
    return jax.shard_map(
        on_device,
        mesh=mesh,
        in_specs=(
            P("fs", "cp", None),
            P("fs", "cp", None),
            P("fs", "cp", None),
            P("fs", "cp", None),
            P("fs", "cp"),
            P("fs", "cp", None),
            P(("cp", "fs"), None),
            P(("cp", "fs"), None),
            P(("cp", "fs"), None),
            P(("cp", "fs"), None),
        ),
        out_specs=(
            P(("cp", "fs"), None),
            P(("cp", "fs"), None),
            P(("cp", "fs"), None),
            P(("cp", "fs"), None),
        ),
        check_vma=False,
    )
```

```python
import math

import jax
import jax.numpy as jnp
from jax import lax
from jax.experimental import pallas as pl
from jax.experimental.pallas import tpu as pltpu
from jax.sharding import PartitionSpec as P

HEAD = 128
KV_HEADS = 4
WIN = 4
GROUP = 4


NORM_EPS = 0.01
MOMENT_DECAY = 0.95
LEARN_RATE = 0.005
WEIGHT_DECAY = 0.1
ADAM_EPS = 1e-08
AVERAGE_MIX = 0.25
INTERP_BETA = 0.9


MESH = pl.DeviceIdType.MESH
VMEM_LIMIT = 60 * 1024 * 1024


def signal_and_wait(peers):
    barrier = pltpu.get_barrier_semaphore()
    for peer in peers:
        pl.semaphore_signal(barrier, inc=1, device_id=peer, device_id_type=MESH)
    pl.semaphore_wait(barrier, len(peers))


def remote(src, dst, send_sem, recv_sem, peer):
    return pltpu.make_async_remote_copy(
        src_ref=src,
        dst_ref=dst,
        send_sem=send_sem,
        recv_sem=recv_sem,
        device_id=peer,
        device_id_type=MESH,
    )


class Place:
    def __init__(self, cp_count, fs_count):
        self.n, self.m = cp_count, fs_count
        self.c, self.f = lax.axis_index("cp"), lax.axis_index("fs")
        self.pair, self.side = self.c // 2, self.c % 2
        self.half = cp_count // 2
        self.mate_c = self.c + 1 - 2 * self.side
        self.twin_f = self.f + 1 - 2 * (self.f % 2)
        self.mate = {"cp": self.mate_c, "fs": self.f}
        self.twin = {"cp": self.c, "fs": self.twin_f}

    def column_c(self, step):
        return ((self.pair + step) % self.half) * 2 + self.side

    def column(self, step):
        return {"cp": self.column_c(step), "fs": self.f}

    def across_f(self, step):
        return (self.f + 2 * step) % self.m

    def across(self, step):
        return {"cp": self.c, "fs": self.across_f(step)}

    def columns(self):
        return [self.column(d) for d in range(1, self.half)]

    def acrosses(self):
        return [self.across(e) for e in range(1, self.m // 2)]


class Window:
    def __init__(self, place, own, win, send, recv):
        self.p, self.own, self.win, self.send, self.recv = place, own, win, send, recv
        self.rows = own.shape[0]

    def slot(self, back):
        return self.win.at[pl.ds((WIN - back) * self.rows, self.rows)]

    def ahead(self, back):
        p = self.p
        peer = {"cp": jnp.minimum(p.c + back, p.n - 1), "fs": p.f}
        return remote(self.own, self.slot(back), self.send.at[back - 1], self.recv.at[back - 1], peer)

    def to_mate(self, source, back):
        return remote(source, self.slot(back), self.send.at[back - 1], self.recv.at[back - 1], self.p.mate)

    def begin(self):
        p = self.p
        for back in (4, 2):

            @pl.when(p.c + back < p.n)
            def _():
                self.ahead(back).start()

        @pl.when(p.side == 0)
        def _():
            self.to_mate(self.own, 1).start()

    def fill(self):
        p = self.p
        self.win[pl.ds(WIN * self.rows, self.rows), :] = self.own[...]
        for back in range(1, WIN + 1):

            @pl.when(p.c < back)
            def _():
                self.win[pl.ds((WIN - back) * self.rows, self.rows), :] = jnp.zeros(
                    self.own.shape, self.own.dtype
                )

    def relay(self):
        p = self.p

        @pl.when(p.c >= 2)
        def _():
            self.ahead(2).wait_recv()

        @pl.when((p.c >= 2) & (p.side == 1))
        def _():
            self.to_mate(self.slot(2), 1).start()

        @pl.when((p.c >= 2) & (p.side == 0))
        def _():
            self.to_mate(self.slot(2), 3).start()

        @pl.when(p.c >= 4)
        def _():
            self.ahead(4).wait_recv()

        @pl.when((p.c >= 4) & (p.side == 1))
        def _():
            self.to_mate(self.slot(4), 3).start()

    def end(self):
        p = self.p
        for back in (1, 3):

            @pl.when(p.c >= back)
            def _():
                self.to_mate(self.own, back).wait_recv()

        for back in (2, 4):

            @pl.when(p.c + back < p.n)
            def _():
                self.ahead(back).wait_send()

        @pl.when((p.side == 0) | (p.c >= 2))
        def _():
            self.to_mate(self.own, 1).wait_send()

        @pl.when(((p.side == 0) & (p.c >= 2)) | (p.c >= 4))
        def _():
            self.to_mate(self.own, 3).wait_send()


def weight_kernel(n, m, y_ref, k_ref, full_ref, win_ref, send, recv, wsend, wrecv):
    p = Place(n, m)
    rows = y_ref.shape[0]
    half, far = n // 2, m // 2
    signal_and_wait(p.columns() + [p.mate] + p.acrosses() + [p.twin])

    def slot(c, f):
        return full_ref.at[pl.ds(pl.multiple_of((c * m + f) * rows, rows), rows)]

    mate_base = half
    across_base = mate_base + half
    twin_base = across_base + (far - 1) * n
    pending = []

    def push(source, c, f, number, peer):
        copy = remote(source, slot(c, f), send.at[number], recv.at[number], peer)
        copy.start()
        pending.append(copy)

    def arrive(c, f, number):
        remote(slot(c, f), slot(c, f), send.at[number], recv.at[number], p.mate).wait_recv()

    def spread(source, c, order):
        for e in range(1, far):
            push(source, c, p.f, across_base + (e - 1) * n + order, p.across(e))
        push(source, c, p.f, twin_base + order, p.twin)

    for d in range(1, half):
        push(y_ref, p.c, p.f, d, p.column(d))
    push(y_ref, p.c, p.f, mate_base, p.mate)
    spread(y_ref, p.c, 0)
    window = Window(p, k_ref, win_ref, wsend, wrecv)
    window.begin()
    full_ref[pl.ds(pl.multiple_of((p.c * m + p.f) * rows, rows), rows), :] = y_ref[...]
    window.fill()
    for d in range(half):
        if d > 0:
            from_c = p.column_c(half - d)
            arrive(from_c, p.f, d)
            push(slot(from_c, p.f), from_c, p.f, mate_base + d, p.mate)
            spread(slot(from_c, p.f), from_c, 2 * d)
        mate_c = p.column_c(half - d) + 1 - 2 * p.side
        arrive(mate_c, p.f, mate_base + d)
        spread(slot(mate_c, p.f), mate_c, 2 * d + 1)
    window.relay()

    def ordered(order):
        from_c = p.column_c((half - order // 2) % half)
        return from_c if order % 2 == 0 else from_c + 1 - 2 * p.side

    for order in range(n):
        c = ordered(order)
        for e in range(1, far):
            g = (p.f + m - 2 * e) % m
            number = across_base + (e - 1) * n + order
            arrive(c, g, number)
            push(slot(c, g), c, g, twin_base + n + (e - 1) * n + order, p.twin)
    for order in range(n):
        c = ordered(order)
        arrive(c, p.twin_f, twin_base + order)
        for e in range(1, far):
            g = (p.twin_f + m - 2 * e) % m
            arrive(c, g, twin_base + n + (e - 1) * n + order)
    window.end()
    for copy in pending:
        copy.wait_send()


def gather_weight(y_weight, keys, n, m):
    rows, width = y_weight.shape
    tok_rows = keys.shape[0]
    numbers = n + (m // 2 - 1) * n + (m // 2) * n
    return pl.pallas_call(
        lambda *refs: weight_kernel(n, m, *refs),
        out_shape=(
            jax.ShapeDtypeStruct((rows * n * m, width), y_weight.dtype),
            jax.ShapeDtypeStruct(((WIN + 1) * tok_rows, width), keys.dtype),
        ),
        in_specs=[pl.BlockSpec(memory_space=pltpu.VMEM)] * 2,
        out_specs=(pl.BlockSpec(memory_space=pltpu.VMEM),) * 2,
        scratch_shapes=[
            pltpu.SemaphoreType.DMA((numbers,)),
            pltpu.SemaphoreType.DMA((numbers,)),
            pltpu.SemaphoreType.DMA((WIN,)),
            pltpu.SemaphoreType.DMA((WIN,)),
        ],
        compiler_params=pltpu.CompilerParams(
            collective_id=1, has_side_effects=True, vmem_limit_bytes=VMEM_LIMIT
        ),
        name="gather_weight",
    )(y_weight, keys)


def attend_kernel(
    n,
    m,
    token_total,
    q_ref,
    cot_ref,
    doc_ref,
    listed_ref,
    kwin_ref,
    v_ref,
    e_ref,
    cols_ref,
    all_ref,
    vwin,
    bias,
    probs,
    att,
    outg,
    own,
    share,
    got,
    csend,
    crecv,
    wsend,
    wrecv,
    send,
    recv,
    gsend,
    grecv,
):
    p = Place(n, m)
    strips, _, _, wide = cols_ref.shape
    tok_rows, span_rows = bias.shape
    heads = KV_HEADS * GROUP
    far = m // 2
    others = [{"cp": p.c, "fs": (p.f + e) % m} for e in range(1, m)]
    around = []
    for back in range(1, WIN + 1):
        around.append({"cp": (p.c + back) % n, "fs": p.f})
        around.append({"cp": (p.c + n - back) % n, "fs": p.f})
    signal_and_wait(around + others)
    window = Window(p, v_ref, vwin, wsend, wrecv)
    window.begin()

    def strip(k, f):
        return pl.ds(pl.multiple_of((k * m + f) * wide, wide), wide)

    def lanes(h):
        return pl.ds(pl.multiple_of(h * HEAD, HEAD), HEAD)

    pending = []
    for k in range(strips):
        for e in range(1, m):
            number = k * (m - 1) + e - 1
            copy = remote(
                e_ref.at[:, strip(k, (p.f + e) % m)],
                cols_ref.at[k, p.f],
                csend.at[number],
                crecv.at[number],
                others[e - 1],
            )
            copy.start()
            pending.append(copy)
    window.fill()
    for k in range(strips):
        cols_ref[k, p.f] = e_ref[:, strip(k, p.f)]
    for back in range(1, WIN + 1):

        @pl.when(p.c + back >= n)
        def _():
            got[back - 1] = jnp.zeros(got.shape[1:], got.dtype)

    row = lax.broadcasted_iota(jnp.int32, (tok_rows, span_rows), 0)
    col = lax.broadcasted_iota(jnp.int32, (tok_rows, span_rows), 1)
    key_pos = (p.c - WIN) * tok_rows + col
    seen = (key_pos >= doc_ref[...]) & (key_pos <= p.c * tok_rows + row) & (listed_ref[...] > 0)
    bias[...] = jnp.where(seen, 0.0, -1e30)
    rate = math.log2(math.e) / math.sqrt(HEAD)

    def prob_step(h, carry):
        raw = (
            lax.dot_general(
                q_ref[:, lanes(h)],
                kwin_ref[:, lanes(h // GROUP)],
                (((1,), (1,)), ((), ())),
                preferred_element_type=jnp.float32,
            )
            + bias[...]
        )
        weights = jnp.exp2((raw - jnp.max(raw, axis=1, keepdims=True)) * rate)
        probs[h] = (weights * (1.0 / jnp.sum(weights, axis=1, keepdims=True))).astype(probs.dtype)
        return carry

    lax.fori_loop(0, heads * 5 // 8, prob_step, 0)
    window.relay()
    lax.fori_loop(heads * 5 // 8, heads, prob_step, 0)
    window.end()

    def out_step(h, carry):
        att[:, lanes(h)] = jnp.dot(
            probs[h], vwin[:, lanes(h // GROUP)], preferred_element_type=jnp.float32
        )
        return carry

    lax.fori_loop(0, heads, out_step, 0)
    tile = 32

    def norm_step(i, carry):
        rows = pl.ds(pl.multiple_of(i * tile, tile), tile)
        attended = att[rows, :]
        inverse = 1.0 / jnp.sqrt(jnp.mean(attended * attended, axis=1, keepdims=True) + NORM_EPS)
        normed = attended * inverse
        upstream = cot_ref[rows, :].astype(jnp.float32) * (1.0 / token_total)
        inner = jnp.mean(upstream * normed, axis=1, keepdims=True)
        outg[rows, :] = ((upstream - normed * inner) * inverse).astype(outg.dtype)
        return carry

    lax.fori_loop(0, tok_rows // tile, norm_step, 0)

    def send_share(kv, back):
        cut = pl.ds(kv * HEAD, HEAD)
        peer = {"cp": jnp.maximum(p.c - back, 0), "fs": p.f}
        number = kv * WIN + back - 1
        return remote(
            share.at[back - 1, :, cut], got.at[back - 1, :, cut], send.at[number], recv.at[number], peer
        )

    for kv in range(KV_HEADS):
        total = None
        for h in range(kv * GROUP, (kv + 1) * GROUP):
            term = lax.dot_general(
                outg[:, h * HEAD : (h + 1) * HEAD],
                probs[h],
                (((0,), (0,)), ((), ())),
                preferred_element_type=jnp.float32,
            )
            total = term if total is None else total + term
        cut = slice(kv * HEAD, (kv + 1) * HEAD)
        for back in range(WIN, -1, -1):
            first = (WIN - back) * tok_rows
            block = total[:, first : first + tok_rows].T
            if back == 0:
                own[:, cut] = block
            else:
                share[back - 1, :, cut] = block.astype(share.dtype)

                @pl.when(p.c >= back)
                def _():
                    send_share(kv, back).start()

    def spread(f, kv, number, peer):
        piece = all_ref.at[f, :, pl.ds(kv * HEAD, HEAD)]
        return remote(piece, piece, gsend.at[number], grecv.at[number], peer)

    for kv in range(KV_HEADS):
        base = kv * (2 * far - 1)
        cut = slice(kv * HEAD, (kv + 1) * HEAD)
        for back in range(1, WIN + 1):

            @pl.when(p.c + back < n)
            def _():
                send_share(kv, back).wait_recv()

        total = own[:, cut]
        for back in range(1, WIN + 1):
            total = total + got[back - 1, :, cut].astype(jnp.float32)
        all_ref[p.f, :, cut] = total.astype(all_ref.dtype)
        for e in range(1, far):
            pending.append(spread(p.f, kv, base + e - 1, p.across(e)))
            pending[-1].start()
        pending.append(spread(p.f, kv, base + far - 1, p.twin))
        pending[-1].start()
    for kv in range(KV_HEADS):
        base = kv * (2 * far - 1)
        for e in range(1, far):
            g = (p.f + m - 2 * e) % m
            spread(g, kv, base + e - 1, p.twin).wait_recv()
            pending.append(spread(g, kv, base + far - 1 + e, p.twin))
            pending[-1].start()
    for kv in range(KV_HEADS):
        base = kv * (2 * far - 1)
        for e in range(far):
            g = (p.twin_f + m - 2 * e) % m
            spread(g, kv, base + far - 1 + e, p.twin).wait_recv()
    for k in range(strips):
        for e in range(1, m):
            g = (p.f + m - e) % m
            number = k * (m - 1) + e - 1
            remote(
                cols_ref.at[k, g], cols_ref.at[k, g], csend.at[number], crecv.at[number], others[0]
            ).wait_recv()
    for copy in pending:
        copy.wait_send()
    for kv in range(KV_HEADS):
        for back in range(1, WIN + 1):

            @pl.when(p.c >= back)
            def _():
                send_share(kv, back).wait_send()


def attend(queries, cots, doc, listed, key_window, values, embeds, strips, wide, n, m):
    tok_rows, width = values.shape
    span_rows = (WIN + 1) * tok_rows
    heads = KV_HEADS * GROUP
    copies = strips * (m - 1)
    gathers = KV_HEADS * (m - 1)
    dma = pltpu.SemaphoreType.DMA
    low = jnp.bfloat16
    return pl.pallas_call(
        lambda *refs: attend_kernel(n, m, tok_rows * n * m, *refs),
        out_shape=(
            jax.ShapeDtypeStruct((strips, m, tok_rows, wide), embeds.dtype),
            jax.ShapeDtypeStruct((m, tok_rows, width), low),
        ),
        in_specs=[pl.BlockSpec(memory_space=pltpu.VMEM)] * 7,
        out_specs=(pl.BlockSpec(memory_space=pltpu.VMEM),) * 2,
        scratch_shapes=[
            pltpu.VMEM((span_rows, width), low),
            pltpu.VMEM((tok_rows, span_rows), jnp.float32),
            pltpu.VMEM((heads, tok_rows, span_rows), low),
            pltpu.VMEM((tok_rows, heads * HEAD), jnp.float32),
            pltpu.VMEM((tok_rows, heads * HEAD), low),
            pltpu.VMEM((tok_rows, width), jnp.float32),
            pltpu.VMEM((WIN, tok_rows, width), low),
            pltpu.VMEM((WIN, tok_rows, width), low),
            dma((copies,)),
            dma((copies,)),
            dma((WIN,)),
            dma((WIN,)),
            dma((KV_HEADS * WIN,)),
            dma((KV_HEADS * WIN,)),
            dma((gathers,)),
            dma((gathers,)),
        ],
        compiler_params=pltpu.CompilerParams(
            collective_id=2, has_side_effects=True, vmem_limit_bytes=VMEM_LIMIT
        ),
        name="attend",
    )(queries, cots, doc, listed, key_window, values, embeds)


def reduce_kernel(n, m, part_ref, out_ref, mate_got, sums, got, msend, mrecv, send, recv):
    p = Place(n, m)
    half = n // 2
    signal_and_wait(p.columns() + [p.mate])

    def to_mate(d):
        target = p.column_c(d) + 1 - 2 * p.side
        return remote(part_ref.at[target], mate_got.at[d], msend.at[d], mrecv.at[d], p.mate)

    def to_owner(d):
        return remote(sums.at[d], got.at[d], send.at[d], recv.at[d], p.column(d))

    steps = list(range(half // 2, half)) + list(range(half // 2 - 1, 0, -1)) + [0]
    for d in steps:
        to_mate(d).start()
    for d in steps:
        to_mate(d).wait_recv()
        both = part_ref[p.column_c(d)].astype(jnp.float32) + mate_got[d].astype(jnp.float32)
        if d > 0:
            sums[d] = both.astype(sums.dtype)
            to_owner(d).start()
        else:
            total = both
    for d in range(1, half):
        to_owner(d).wait_recv()
        total = total + got[d].astype(jnp.float32)
    out_ref[...] = total
    for d in range(half):
        to_mate(d).wait_send()
    for d in range(1, half):
        to_owner(d).wait_send()


def reduce_parts(parts, n, m):
    _, rows, width = parts.shape
    half = n // 2
    return pl.pallas_call(
        lambda *refs: reduce_kernel(n, m, *refs),
        out_shape=jax.ShapeDtypeStruct((rows, width), jnp.float32),
        in_specs=[pl.BlockSpec(memory_space=pltpu.VMEM)],
        out_specs=pl.BlockSpec(memory_space=pltpu.VMEM),
        scratch_shapes=[pltpu.VMEM((half, rows, width), parts.dtype)] * 3
        + [pltpu.SemaphoreType.DMA((half,))] * 4,
        compiler_params=pltpu.CompilerParams(
            collective_id=4, has_side_effects=True, vmem_limit_bytes=VMEM_LIMIT
        ),
        name="reduce_parts",
    )(parts)


def listed_keys(need_row, block_id, tok_rows):
    span_rows = (WIN + 1) * tok_rows
    key_block = block_id - WIN + jnp.arange(span_rows, dtype=jnp.int32) // tok_rows
    return jnp.any(need_row[None, :] == key_block[:, None], axis=1).astype(jnp.int32)[None, :]


def on_device(
    embeds,
    queries,
    key_heads,
    cotangent,
    doc_start,
    need_ids,
    y_weight,
    z_weight,
    x_weight,
    second_moment,
):
    tokens_here = embeds[0]
    tok_rows = tokens_here.shape[0]
    kv_width = key_heads.shape[2]
    block_id = lax.axis_index("cp")
    n, m = lax.axis_size("cp"), lax.axis_size("fs")
    own_rows = y_weight.shape[0]
    full_weight, key_window = gather_weight(y_weight, key_heads[0], n, m)
    values = jnp.dot(tokens_here, full_weight, preferred_element_type=jnp.float32).astype(
        jnp.bfloat16
    )
    if own_rows % 128 == 0:
        strips, wide, sent_cols = n, own_rows, tokens_here
    else:
        strips, wide = 1, n * own_rows
        sent_cols = (
            tokens_here.reshape(tok_rows, n, m, own_rows)
            .transpose(0, 2, 1, 3)
            .reshape(tok_rows, n * m * own_rows)
        )
    group_cols, group_grads = attend(
        queries[0],
        cotangent[0],
        doc_start[0][:, None],
        listed_keys(need_ids[0, 0], block_id, tok_rows),
        key_window,
        values,
        sent_cols,
        strips,
        wide,
        n,
        m,
    )
    parts = jnp.einsum(
        "stw,te->swe",
        group_cols.reshape(strips, m * tok_rows, wide),
        group_grads.reshape(m * tok_rows, kv_width),
        preferred_element_type=jnp.float32,
    ).astype(jnp.bfloat16)
    gradient = reduce_parts(parts.reshape(n, own_rows, kv_width), n, m)
    moment_next = MOMENT_DECAY * second_moment + (1.0 - MOMENT_DECAY) * gradient * gradient
    z_next = z_weight - LEARN_RATE * (
        gradient / (jnp.sqrt(moment_next) + ADAM_EPS) + WEIGHT_DECAY * y_weight.astype(jnp.float32)
    )
    x_next = (1.0 - AVERAGE_MIX) * x_weight + AVERAGE_MIX * z_next
    y_next = ((1.0 - INTERP_BETA) * z_next + INTERP_BETA * x_next).astype(jnp.bfloat16)
    return (z_next, x_next, moment_next, y_next)


def solution(mesh):
    return jax.shard_map(
        on_device,
        mesh=mesh,
        in_specs=(
            P("fs", "cp", None),
            P("fs", "cp", None),
            P("fs", "cp", None),
            P("fs", "cp", None),
            P("fs", "cp"),
            P("fs", "cp", None),
            P(("cp", "fs"), None),
            P(("cp", "fs"), None),
            P(("cp", "fs"), None),
            P(("cp", "fs"), None),
        ),
        out_specs=(
            P(("cp", "fs"), None),
            P(("cp", "fs"), None),
            P(("cp", "fs"), None),
            P(("cp", "fs"), None),
        ),
        check_vma=False,
    )
```

```python
import math

import jax
import jax.numpy as jnp
from jax import lax
from jax.experimental import pallas as pl
from jax.experimental.pallas import tpu as pltpu
from jax.sharding import PartitionSpec as P

HEAD = 128
KV_HEADS = 4
WIN = 4
GROUP = 4


NORM_EPS = 0.01
MOMENT_DECAY = 0.95
LEARN_RATE = 0.005
WEIGHT_DECAY = 0.1
ADAM_EPS = 1e-08
AVERAGE_MIX = 0.25
INTERP_BETA = 0.9


MESH = pl.DeviceIdType.MESH
VMEM_LIMIT = 60 * 1024 * 1024


def signal_and_wait(peers):
    barrier = pltpu.get_barrier_semaphore()
    for peer in peers:
        pl.semaphore_signal(barrier, inc=1, device_id=peer, device_id_type=MESH)
    pl.semaphore_wait(barrier, len(peers))


def remote(src, dst, send_sem, recv_sem, peer):
    return pltpu.make_async_remote_copy(
        src_ref=src,
        dst_ref=dst,
        send_sem=send_sem,
        recv_sem=recv_sem,
        device_id=peer,
        device_id_type=MESH,
    )


class Place:
    def __init__(self, cp_count, fs_count):
        self.n, self.m = cp_count, fs_count
        self.c, self.f = lax.axis_index("cp"), lax.axis_index("fs")
        self.pair, self.side = self.c // 2, self.c % 2
        self.half = cp_count // 2
        self.mate_c = self.c + 1 - 2 * self.side
        self.twin_f = self.f + 1 - 2 * (self.f % 2)
        self.mate = {"cp": self.mate_c, "fs": self.f}
        self.twin = {"cp": self.c, "fs": self.twin_f}

    def column_c(self, step):
        return ((self.pair + step) % self.half) * 2 + self.side

    def column(self, step):
        return {"cp": self.column_c(step), "fs": self.f}

    def across_f(self, step):
        return (self.f + 2 * step) % self.m

    def across(self, step):
        return {"cp": self.c, "fs": self.across_f(step)}

    def columns(self):
        return [self.column(d) for d in range(1, self.half)]

    def acrosses(self):
        return [self.across(e) for e in range(1, self.m // 2)]


class Window:
    def __init__(self, place, own, win, send, recv):
        self.p, self.own, self.win, self.send, self.recv = place, own, win, send, recv
        self.rows = own.shape[0]

    def slot(self, back):
        return self.win.at[pl.ds((WIN - back) * self.rows, self.rows)]

    def ahead(self, back):
        p = self.p
        peer = {"cp": jnp.minimum(p.c + back, p.n - 1), "fs": p.f}
        return remote(self.own, self.slot(back), self.send.at[back - 1], self.recv.at[back - 1], peer)

    def to_mate(self, source, back):
        return remote(source, self.slot(back), self.send.at[back - 1], self.recv.at[back - 1], self.p.mate)

    def begin(self):
        p = self.p
        for back in (4, 2):

            @pl.when(p.c + back < p.n)
            def _():
                self.ahead(back).start()

        @pl.when(p.side == 0)
        def _():
            self.to_mate(self.own, 1).start()

    def fill(self):
        p = self.p
        self.win[pl.ds(WIN * self.rows, self.rows), :] = self.own[...]
        for back in range(1, WIN + 1):

            @pl.when(p.c < back)
            def _():
                self.win[pl.ds((WIN - back) * self.rows, self.rows), :] = jnp.zeros(
                    self.own.shape, self.own.dtype
                )

    def relay(self):
        p = self.p

        @pl.when(p.c >= 2)
        def _():
            self.ahead(2).wait_recv()

        @pl.when((p.c >= 2) & (p.side == 1))
        def _():
            self.to_mate(self.slot(2), 1).start()

        @pl.when((p.c >= 2) & (p.side == 0))
        def _():
            self.to_mate(self.slot(2), 3).start()

        @pl.when(p.c >= 4)
        def _():
            self.ahead(4).wait_recv()

        @pl.when((p.c >= 4) & (p.side == 1))
        def _():
            self.to_mate(self.slot(4), 3).start()

    def end(self):
        p = self.p
        for back in (1, 3):

            @pl.when(p.c >= back)
            def _():
                self.to_mate(self.own, back).wait_recv()

        for back in (2, 4):

            @pl.when(p.c + back < p.n)
            def _():
                self.ahead(back).wait_send()

        @pl.when((p.side == 0) | (p.c >= 2))
        def _():
            self.to_mate(self.own, 1).wait_send()

        @pl.when(((p.side == 0) & (p.c >= 2)) | (p.c >= 4))
        def _():
            self.to_mate(self.own, 3).wait_send()


def weight_kernel(n, m, y_ref, k_ref, full_ref, win_ref, send, recv, wsend, wrecv):
    p = Place(n, m)
    rows = y_ref.shape[0]
    half, far = n // 2, m // 2
    signal_and_wait(p.columns() + [p.mate] + p.acrosses() + [p.twin])

    def slot(c, f):
        return full_ref.at[pl.ds(pl.multiple_of((c * m + f) * rows, rows), rows)]

    mate_base = half
    across_base = mate_base + half
    twin_base = across_base + (far - 1) * n
    pending = []

    def push(source, c, f, number, peer):
        copy = remote(source, slot(c, f), send.at[number], recv.at[number], peer)
        copy.start()
        pending.append(copy)

    def arrive(c, f, number):
        remote(slot(c, f), slot(c, f), send.at[number], recv.at[number], p.mate).wait_recv()

    def spread(source, c, order):
        for e in range(1, far):
            push(source, c, p.f, across_base + (e - 1) * n + order, p.across(e))
        push(source, c, p.f, twin_base + order, p.twin)

    for d in range(1, half):
        push(y_ref, p.c, p.f, d, p.column(d))
    push(y_ref, p.c, p.f, mate_base, p.mate)
    spread(y_ref, p.c, 0)
    window = Window(p, k_ref, win_ref, wsend, wrecv)
    window.begin()
    full_ref[pl.ds(pl.multiple_of((p.c * m + p.f) * rows, rows), rows), :] = y_ref[...]
    window.fill()
    for d in range(half):
        if d > 0:
            from_c = p.column_c(half - d)
            arrive(from_c, p.f, d)
            push(slot(from_c, p.f), from_c, p.f, mate_base + d, p.mate)
            spread(slot(from_c, p.f), from_c, 2 * d)
        mate_c = p.column_c(half - d) + 1 - 2 * p.side
        arrive(mate_c, p.f, mate_base + d)
        spread(slot(mate_c, p.f), mate_c, 2 * d + 1)
    window.relay()

    def ordered(order):
        from_c = p.column_c((half - order // 2) % half)
        return from_c if order % 2 == 0 else from_c + 1 - 2 * p.side

    for order in range(n):
        c = ordered(order)
        for e in range(1, far):
            g = (p.f + m - 2 * e) % m
            number = across_base + (e - 1) * n + order
            arrive(c, g, number)
            push(slot(c, g), c, g, twin_base + n + (e - 1) * n + order, p.twin)
    for order in range(n):
        c = ordered(order)
        arrive(c, p.twin_f, twin_base + order)
        for e in range(1, far):
            g = (p.twin_f + m - 2 * e) % m
            arrive(c, g, twin_base + n + (e - 1) * n + order)
    window.end()
    for copy in pending:
        copy.wait_send()


def gather_weight(y_weight, keys, n, m):
    rows, width = y_weight.shape
    tok_rows = keys.shape[0]
    numbers = n + (m // 2 - 1) * n + (m // 2) * n
    return pl.pallas_call(
        lambda *refs: weight_kernel(n, m, *refs),
        out_shape=(
            jax.ShapeDtypeStruct((rows * n * m, width), y_weight.dtype),
            jax.ShapeDtypeStruct(((WIN + 1) * tok_rows, width), keys.dtype),
        ),
        in_specs=[pl.BlockSpec(memory_space=pltpu.VMEM)] * 2,
        out_specs=(pl.BlockSpec(memory_space=pltpu.VMEM),) * 2,
        scratch_shapes=[
            pltpu.SemaphoreType.DMA((numbers,)),
            pltpu.SemaphoreType.DMA((numbers,)),
            pltpu.SemaphoreType.DMA((WIN,)),
            pltpu.SemaphoreType.DMA((WIN,)),
        ],
        compiler_params=pltpu.CompilerParams(
            collective_id=1, has_side_effects=True, vmem_limit_bytes=VMEM_LIMIT
        ),
        name="gather_weight",
    )(y_weight, keys)


def attend_kernel(
    n,
    m,
    token_total,
    q_ref,
    cot_ref,
    doc_ref,
    listed_ref,
    kwin_ref,
    v_ref,
    e_ref,
    cols_ref,
    all_ref,
    vwin,
    bias,
    probs,
    att,
    outg,
    own,
    share,
    got,
    csend,
    crecv,
    wsend,
    wrecv,
    send,
    recv,
    gsend,
    grecv,
):
    p = Place(n, m)
    strips, _, _, wide = cols_ref.shape
    tok_rows, span_rows = bias.shape
    heads = KV_HEADS * GROUP
    far = m // 2
    others = [{"cp": p.c, "fs": (p.f + e) % m} for e in range(1, m)]
    around = []
    for back in range(1, WIN + 1):
        around.append({"cp": (p.c + back) % n, "fs": p.f})
        around.append({"cp": (p.c + n - back) % n, "fs": p.f})
    signal_and_wait(around + others)
    window = Window(p, v_ref, vwin, wsend, wrecv)
    window.begin()

    def strip(k, f):
        return pl.ds(pl.multiple_of((k * m + f) * wide, wide), wide)

    def lanes(h):
        return pl.ds(pl.multiple_of(h * HEAD, HEAD), HEAD)

    pending = []
    for k in range(strips):
        for e in range(1, m):
            number = k * (m - 1) + e - 1
            copy = remote(
                e_ref.at[:, strip(k, (p.f + e) % m)],
                cols_ref.at[k, p.f],
                csend.at[number],
                crecv.at[number],
                others[e - 1],
            )
            copy.start()
            pending.append(copy)
    window.fill()
    for k in range(strips):
        cols_ref[k, p.f] = e_ref[:, strip(k, p.f)]
    for back in range(1, WIN + 1):

        @pl.when(p.c + back >= n)
        def _():
            got[back - 1] = jnp.zeros(got.shape[1:], got.dtype)

    row = lax.broadcasted_iota(jnp.int32, (tok_rows, span_rows), 0)
    col = lax.broadcasted_iota(jnp.int32, (tok_rows, span_rows), 1)
    key_pos = (p.c - WIN) * tok_rows + col
    seen = (key_pos >= doc_ref[...]) & (key_pos <= p.c * tok_rows + row) & (listed_ref[...] > 0)
    bias[...] = jnp.where(seen, 0.0, -1e30)
    rate = math.log2(math.e) / math.sqrt(HEAD)

    def prob_step(h, carry):
        raw = (
            lax.dot_general(
                q_ref[:, lanes(h)],
                kwin_ref[:, lanes(h // GROUP)],
                (((1,), (1,)), ((), ())),
                preferred_element_type=jnp.float32,
            )
            + bias[...]
        )
        weights = jnp.exp2((raw - jnp.max(raw, axis=1, keepdims=True)) * rate)
        probs[h] = (weights * (1.0 / jnp.sum(weights, axis=1, keepdims=True))).astype(probs.dtype)
        return carry

    lax.fori_loop(0, heads * 5 // 8, prob_step, 0, unroll=2)
    window.relay()
    lax.fori_loop(heads * 5 // 8, heads, prob_step, 0, unroll=2)
    window.end()

    def out_step(h, carry):
        att[:, lanes(h)] = jnp.dot(
            probs[h], vwin[:, lanes(h // GROUP)], preferred_element_type=jnp.float32
        )
        return carry

    lax.fori_loop(0, heads, out_step, 0, unroll=4)
    tile = 32

    def norm_step(i, carry):
        rows = pl.ds(pl.multiple_of(i * tile, tile), tile)
        attended = att[rows, :]
        inverse = 1.0 / jnp.sqrt(jnp.mean(attended * attended, axis=1, keepdims=True) + NORM_EPS)
        normed = attended * inverse
        upstream = cot_ref[rows, :].astype(jnp.float32) * (1.0 / token_total)
        inner = jnp.mean(upstream * normed, axis=1, keepdims=True)
        outg[rows, :] = ((upstream - normed * inner) * inverse).astype(outg.dtype)
        return carry

    lax.fori_loop(0, tok_rows // tile, norm_step, 0)

    def send_share(kv, back):
        cut = pl.ds(kv * HEAD, HEAD)
        peer = {"cp": jnp.maximum(p.c - back, 0), "fs": p.f}
        number = kv * WIN + back - 1
        return remote(
            share.at[back - 1, :, cut], got.at[back - 1, :, cut], send.at[number], recv.at[number], peer
        )

    for kv in range(KV_HEADS):
        total = None
        for h in range(kv * GROUP, (kv + 1) * GROUP):
            term = lax.dot_general(
                outg[:, h * HEAD : (h + 1) * HEAD],
                probs[h],
                (((0,), (0,)), ((), ())),
                preferred_element_type=jnp.float32,
            )
            total = term if total is None else total + term
        cut = slice(kv * HEAD, (kv + 1) * HEAD)
        for back in range(WIN, -1, -1):
            first = (WIN - back) * tok_rows
            block = total[:, first : first + tok_rows].T
            if back == 0:
                own[:, cut] = block
            else:
                share[back - 1, :, cut] = block.astype(share.dtype)

                @pl.when(p.c >= back)
                def _():
                    send_share(kv, back).start()

    def spread(f, kv, number, peer):
        piece = all_ref.at[f, :, pl.ds(kv * HEAD, HEAD)]
        return remote(piece, piece, gsend.at[number], grecv.at[number], peer)

    for kv in range(KV_HEADS):
        base = kv * (2 * far - 1)
        cut = slice(kv * HEAD, (kv + 1) * HEAD)
        for back in range(1, WIN + 1):

            @pl.when(p.c + back < n)
            def _():
                send_share(kv, back).wait_recv()

        total = own[:, cut]
        for back in range(1, WIN + 1):
            total = total + got[back - 1, :, cut].astype(jnp.float32)
        all_ref[p.f, :, cut] = total.astype(all_ref.dtype)
        for e in range(1, far):
            pending.append(spread(p.f, kv, base + e - 1, p.across(e)))
            pending[-1].start()
        pending.append(spread(p.f, kv, base + far - 1, p.twin))
        pending[-1].start()
    for kv in range(KV_HEADS):
        base = kv * (2 * far - 1)
        for e in range(1, far):
            g = (p.f + m - 2 * e) % m
            spread(g, kv, base + e - 1, p.twin).wait_recv()
            pending.append(spread(g, kv, base + far - 1 + e, p.twin))
            pending[-1].start()
    for kv in range(KV_HEADS):
        base = kv * (2 * far - 1)
        for e in range(far):
            g = (p.twin_f + m - 2 * e) % m
            spread(g, kv, base + far - 1 + e, p.twin).wait_recv()
    for k in range(strips):
        for e in range(1, m):
            g = (p.f + m - e) % m
            number = k * (m - 1) + e - 1
            remote(
                cols_ref.at[k, g], cols_ref.at[k, g], csend.at[number], crecv.at[number], others[0]
            ).wait_recv()
    for copy in pending:
        copy.wait_send()
    for kv in range(KV_HEADS):
        for back in range(1, WIN + 1):

            @pl.when(p.c >= back)
            def _():
                send_share(kv, back).wait_send()


def attend(queries, cots, doc, listed, key_window, values, embeds, strips, wide, n, m):
    tok_rows, width = values.shape
    span_rows = (WIN + 1) * tok_rows
    heads = KV_HEADS * GROUP
    copies = strips * (m - 1)
    gathers = KV_HEADS * (m - 1)
    dma = pltpu.SemaphoreType.DMA
    low = jnp.bfloat16
    return pl.pallas_call(
        lambda *refs: attend_kernel(n, m, tok_rows * n * m, *refs),
        out_shape=(
            jax.ShapeDtypeStruct((strips, m, tok_rows, wide), embeds.dtype),
            jax.ShapeDtypeStruct((m, tok_rows, width), low),
        ),
        in_specs=[pl.BlockSpec(memory_space=pltpu.VMEM)] * 7,
        out_specs=(pl.BlockSpec(memory_space=pltpu.VMEM),) * 2,
        scratch_shapes=[
            pltpu.VMEM((span_rows, width), low),
            pltpu.VMEM((tok_rows, span_rows), jnp.float32),
            pltpu.VMEM((heads, tok_rows, span_rows), low),
            pltpu.VMEM((tok_rows, heads * HEAD), jnp.float32),
            pltpu.VMEM((tok_rows, heads * HEAD), low),
            pltpu.VMEM((tok_rows, width), jnp.float32),
            pltpu.VMEM((WIN, tok_rows, width), low),
            pltpu.VMEM((WIN, tok_rows, width), low),
            dma((copies,)),
            dma((copies,)),
            dma((WIN,)),
            dma((WIN,)),
            dma((KV_HEADS * WIN,)),
            dma((KV_HEADS * WIN,)),
            dma((gathers,)),
            dma((gathers,)),
        ],
        compiler_params=pltpu.CompilerParams(
            collective_id=2, has_side_effects=True, vmem_limit_bytes=VMEM_LIMIT
        ),
        name="attend",
    )(queries, cots, doc, listed, key_window, values, embeds)


def reduce_kernel(n, m, part_ref, out_ref, mate_got, sums, got, msend, mrecv, send, recv):
    p = Place(n, m)
    half = n // 2
    signal_and_wait(p.columns() + [p.mate])

    def to_mate(d):
        target = p.column_c(d) + 1 - 2 * p.side
        return remote(part_ref.at[target], mate_got.at[d], msend.at[d], mrecv.at[d], p.mate)

    def to_owner(d):
        return remote(sums.at[d], got.at[d], send.at[d], recv.at[d], p.column(d))

    steps = list(range(half // 2, half)) + list(range(half // 2 - 1, 0, -1)) + [0]
    for d in steps:
        to_mate(d).start()
    for d in steps:
        to_mate(d).wait_recv()
        both = part_ref[p.column_c(d)].astype(jnp.float32) + mate_got[d].astype(jnp.float32)
        if d > 0:
            sums[d] = both.astype(sums.dtype)
            to_owner(d).start()
        else:
            total = both
    for d in range(1, half):
        to_owner(d).wait_recv()
        total = total + got[d].astype(jnp.float32)
    out_ref[...] = total
    for d in range(half):
        to_mate(d).wait_send()
    for d in range(1, half):
        to_owner(d).wait_send()


def reduce_parts(parts, n, m):
    _, rows, width = parts.shape
    half = n // 2
    return pl.pallas_call(
        lambda *refs: reduce_kernel(n, m, *refs),
        out_shape=jax.ShapeDtypeStruct((rows, width), jnp.float32),
        in_specs=[pl.BlockSpec(memory_space=pltpu.VMEM)],
        out_specs=pl.BlockSpec(memory_space=pltpu.VMEM),
        scratch_shapes=[pltpu.VMEM((half, rows, width), parts.dtype)] * 3
        + [pltpu.SemaphoreType.DMA((half,))] * 4,
        compiler_params=pltpu.CompilerParams(
            collective_id=4, has_side_effects=True, vmem_limit_bytes=VMEM_LIMIT
        ),
        name="reduce_parts",
    )(parts)


def listed_keys(need_row, block_id, tok_rows):
    span_rows = (WIN + 1) * tok_rows
    key_block = block_id - WIN + jnp.arange(span_rows, dtype=jnp.int32) // tok_rows
    return jnp.any(need_row[None, :] == key_block[:, None], axis=1).astype(jnp.int32)[None, :]


def on_device(
    embeds,
    queries,
    key_heads,
    cotangent,
    doc_start,
    need_ids,
    y_weight,
    z_weight,
    x_weight,
    second_moment,
):
    tokens_here = embeds[0]
    tok_rows = tokens_here.shape[0]
    kv_width = key_heads.shape[2]
    block_id = lax.axis_index("cp")
    n, m = lax.axis_size("cp"), lax.axis_size("fs")
    own_rows = y_weight.shape[0]
    full_weight, key_window = gather_weight(y_weight, key_heads[0], n, m)
    values = jnp.dot(tokens_here, full_weight, preferred_element_type=jnp.float32).astype(
        jnp.bfloat16
    )
    if own_rows % 128 == 0:
        strips, wide, sent_cols = n, own_rows, tokens_here
    else:
        strips, wide = 1, n * own_rows
        sent_cols = (
            tokens_here.reshape(tok_rows, n, m, own_rows)
            .transpose(0, 2, 1, 3)
            .reshape(tok_rows, n * m * own_rows)
        )
    group_cols, group_grads = attend(
        queries[0],
        cotangent[0],
        doc_start[0][:, None],
        listed_keys(need_ids[0, 0], block_id, tok_rows),
        key_window,
        values,
        sent_cols,
        strips,
        wide,
        n,
        m,
    )
    parts = jnp.einsum(
        "stw,te->swe",
        group_cols.reshape(strips, m * tok_rows, wide),
        group_grads.reshape(m * tok_rows, kv_width),
        preferred_element_type=jnp.float32,
    ).astype(jnp.bfloat16)
    gradient = reduce_parts(parts.reshape(n, own_rows, kv_width), n, m)
    moment_next = MOMENT_DECAY * second_moment + (1.0 - MOMENT_DECAY) * gradient * gradient
    z_next = z_weight - LEARN_RATE * (
        gradient / (jnp.sqrt(moment_next) + ADAM_EPS) + WEIGHT_DECAY * y_weight.astype(jnp.float32)
    )
    x_next = (1.0 - AVERAGE_MIX) * x_weight + AVERAGE_MIX * z_next
    y_next = ((1.0 - INTERP_BETA) * z_next + INTERP_BETA * x_next).astype(jnp.bfloat16)
    return (z_next, x_next, moment_next, y_next)


def solution(mesh):
    return jax.shard_map(
        on_device,
        mesh=mesh,
        in_specs=(
            P("fs", "cp", None),
            P("fs", "cp", None),
            P("fs", "cp", None),
            P("fs", "cp", None),
            P("fs", "cp"),
            P("fs", "cp", None),
            P(("cp", "fs"), None),
            P(("cp", "fs"), None),
            P(("cp", "fs"), None),
            P(("cp", "fs"), None),
        ),
        out_specs=(
            P(("cp", "fs"), None),
            P(("cp", "fs"), None),
            P(("cp", "fs"), None),
            P(("cp", "fs"), None),
        ),
        check_vma=False,
    )
```
